8 devices in a mesh: ep: 8 (over z, y, x, core).
Axes of the slice: x: 2, y: 2, z: 1, core: 2. Of those that a mesh axis runs over, the one named last changes fastest.
Arguments:
- x_tokens: bfloat16 [4096, 1536], P('ep')
- w_router: bfloat16 [1536, 64], replicated
- w_gate: bfloat16 [64, 1536, 512], P('ep')
- w_up: bfloat16 [64, 1536, 512], P('ep')
- w_down: bfloat16 [64, 512, 1536], P('ep')
- topk_idx: int32 [4096, 6], P('ep')
- dy_tokens: bfloat16 [4096, 1536], P('ep')
Outputs:
- output 1: bfloat16 [4096, 1536], P('ep')
- output 2: float32 [], replicated
- output 3: bfloat16 [4096, 1536], P('ep')
- output 4: float32 [1536, 64], replicated
- output 5: float32 [64, 1536, 512], P('ep')
- output 6: float32 [64, 1536, 512], P('ep')
- output 7: float32 [64, 512, 1536], P('ep')
All inputs are finite; a program needn't handle non-finite values.
Results may differ from the reference program's by a relative error of at most 0.00533538.
Values are sent between devices in bfloat16 or wider.
A program may use at most 1 GiB of HBM per device.

```python
import jax
import jax.numpy as jnp
from jax import lax

MODEL_DIM = 1536
FF_DIM = 512
NUM_EXPERTS = 64
TOP_K = 6
TOK_PER_DEV = 512
NUM_DEVICES = 8
ALL_TOKENS = NUM_DEVICES * TOK_PER_DEV
CAPACITY = (5 * TOK_PER_DEV * TOP_K + 4 * NUM_EXPERTS - 1) // (4 * NUM_EXPERTS)
AUX_COEF = 0.001


def draw_routing(key):
    bias_key, score_key = jax.random.split(key)
    dev_bias = jax.random.randint(bias_key, (NUM_DEVICES, 1, NUM_EXPERTS), 0, 61)
    scores = jax.random.randint(score_key, (NUM_DEVICES, TOK_PER_DEV, NUM_EXPERTS), 0, 1000)
    ranked = (scores + dev_bias) * NUM_EXPERTS + jnp.arange(NUM_EXPERTS, dtype=jnp.int32)
    chosen = lax.top_k(ranked, TOP_K)[1]
    return chosen.reshape(ALL_TOKENS, TOP_K).astype(jnp.int32)


def setup_inputs(seed: int = 0) -> dict:
    key_list = jax.random.split(jax.random.key(seed), 7)
    topk_idx = draw_routing(key_list[0])
    router_f = jax.random.normal(key_list[1], (MODEL_DIM, NUM_EXPERTS), jnp.float32) * MODEL_DIM ** -0.5
    chosen_hot = jnp.zeros((ALL_TOKENS, NUM_EXPERTS), jnp.float32).at[jnp.arange(ALL_TOKENS)[:, None], topk_idx].set(1.0)
    x_noise = jax.random.normal(key_list[2], (ALL_TOKENS, MODEL_DIM), jnp.float32)
    x_tokens = x_noise + 3.0 * jnp.dot(chosen_hot, router_f.T)
    w_gate = jax.random.normal(key_list[3], (NUM_EXPERTS, MODEL_DIM, FF_DIM), jnp.float32) * MODEL_DIM ** -0.5
    w_up = jax.random.normal(key_list[4], (NUM_EXPERTS, MODEL_DIM, FF_DIM), jnp.float32) * MODEL_DIM ** -0.5
    w_down = jax.random.normal(key_list[5], (NUM_EXPERTS, FF_DIM, MODEL_DIM), jnp.float32) * FF_DIM ** -0.5
    dy_tokens = jax.random.normal(key_list[6], (ALL_TOKENS, MODEL_DIM), jnp.float32)
    return {
        "x_tokens": x_tokens.astype(jnp.bfloat16),
        "w_router": router_f.astype(jnp.bfloat16),
        "w_gate": w_gate.astype(jnp.bfloat16),
        "w_up": w_up.astype(jnp.bfloat16),
        "w_down": w_down.astype(jnp.bfloat16),
        "topk_idx": topk_idx,
        "dy_tokens": dy_tokens.astype(jnp.bfloat16),
    }


def reference(x_tokens, w_router, w_gate, w_up, w_down, topk_idx, dy_tokens):
    logits = jnp.dot(x_tokens, w_router, preferred_element_type=jnp.float32)
    router_prob = jax.nn.softmax(logits, axis=-1)
    counts = jax.ops.segment_sum(jnp.ones((ALL_TOKENS * TOP_K,), jnp.float32), topk_idx.reshape(-1), num_segments=NUM_EXPERTS)
    load_frac = counts / (ALL_TOKENS * TOP_K)
    mean_prob = jnp.mean(router_prob, axis=0)
    aux_loss = AUX_COEF * NUM_EXPERTS * jnp.sum(load_frac * mean_prob)
    aux_grad = AUX_COEF * NUM_EXPERTS * load_frac / ALL_TOKENS
    w_gate32 = w_gate.astype(jnp.float32)
    w_up32 = w_up.astype(jnp.float32)
    w_down32 = w_down.astype(jnp.float32)
    zero_row = jnp.zeros((1, MODEL_DIM), x_tokens.dtype)
    n_slots = NUM_EXPERTS * CAPACITY

    def device_step(carry_acc, dev_in):
        dwg_acc, dwu_acc, dwd_acc, dwr_acc = carry_acc
        x_dev, prob_dev, idx_dev, dy_dev = dev_in
        pick_prob = jnp.take_along_axis(prob_dev, idx_dev, axis=1)
        pick_sum = jnp.sum(pick_prob, axis=1, keepdims=True)
        gate_f32 = pick_prob / pick_sum
        gate_bf = gate_f32.astype(jnp.bfloat16)
        choice_mask = idx_dev[:, :, None] == jnp.arange(NUM_EXPERTS)[None, None, :]
        expert_hot = jnp.sum(choice_mask.astype(jnp.int32), axis=1)
        earlier = jnp.cumsum(expert_hot, axis=0) - expert_hot
        position = jnp.take_along_axis(earlier, idx_dev, axis=1)
        slot_ids = jnp.where(position < CAPACITY, idx_dev * CAPACITY + position, n_slots)
        flat_slots = slot_ids.reshape(-1)
        x_rep = jnp.broadcast_to(x_dev[:, None, :], (TOK_PER_DEV, TOP_K, MODEL_DIM)).reshape(TOK_PER_DEV * TOP_K, MODEL_DIM)
        buf_x = jnp.zeros((n_slots + 1, MODEL_DIM), x_dev.dtype).at[flat_slots].set(x_rep)[:n_slots]
        buf_x32 = buf_x.reshape(NUM_EXPERTS, CAPACITY, MODEL_DIM).astype(jnp.float32)
        gate_pre = jnp.einsum("ecd,edf->ecf", buf_x32, w_gate32)
        up_pre = jnp.einsum("ecd,edf->ecf", buf_x32, w_up32)
        act_gate = jax.nn.silu(gate_pre)
        hidden = (act_gate * up_pre).astype(jnp.bfloat16).astype(jnp.float32)
        out_slot = jnp.einsum("ecf,efd->ecd", hidden, w_down32).astype(jnp.bfloat16)
        out_tok = jnp.concatenate([out_slot.reshape(n_slots, MODEL_DIM), zero_row])[slot_ids]
        y_dev = jnp.sum(gate_bf.astype(jnp.float32)[:, :, None] * out_tok.astype(jnp.float32), axis=1).astype(jnp.bfloat16)
        do_tok = (gate_bf.astype(jnp.float32)[:, :, None] * dy_dev.astype(jnp.float32)[:, None, :]).astype(jnp.bfloat16)
        buf_do = jnp.zeros((n_slots + 1, MODEL_DIM), dy_dev.dtype).at[flat_slots].set(do_tok.reshape(TOK_PER_DEV * TOP_K, MODEL_DIM))[:n_slots]
        buf_do32 = buf_do.reshape(NUM_EXPERTS, CAPACITY, MODEL_DIM).astype(jnp.float32)
        dwd_new = dwd_acc + jnp.einsum("ecf,ecd->efd", hidden, buf_do32)
        d_hidden = jnp.einsum("ecd,efd->ecf", buf_do32, w_down32).astype(jnp.bfloat16).astype(jnp.float32)
        sigmoid_g = jax.nn.sigmoid(gate_pre)
        d_gate_pre = (d_hidden * up_pre * sigmoid_g * (1.0 + gate_pre * (1.0 - sigmoid_g))).astype(jnp.bfloat16).astype(jnp.float32)
        d_up_pre = (d_hidden * act_gate).astype(jnp.bfloat16).astype(jnp.float32)
        dwg_new = dwg_acc + jnp.einsum("ecd,ecf->edf", buf_x32, d_gate_pre)
        dwu_new = dwu_acc + jnp.einsum("ecd,ecf->edf", buf_x32, d_up_pre)
        dx_slot = (jnp.einsum("ecf,edf->ecd", d_gate_pre, w_gate32) + jnp.einsum("ecf,edf->ecd", d_up_pre, w_up32)).astype(jnp.bfloat16)
        dx_tok = jnp.concatenate([dx_slot.reshape(n_slots, MODEL_DIM), zero_row])[slot_ids]
        dx_expert = jnp.sum(dx_tok.astype(jnp.float32), axis=1)
        d_gate = jnp.sum(out_tok.astype(jnp.float32) * dy_dev.astype(jnp.float32)[:, None, :], axis=2)
        d_pick = (d_gate - jnp.sum(d_gate * gate_f32, axis=1, keepdims=True)) / pick_sum
        d_prob = jnp.sum(jnp.where(choice_mask, d_pick[:, :, None], 0.0), axis=1) + aux_grad
        d_logit = prob_dev * (d_prob - jnp.sum(prob_dev * d_prob, axis=1, keepdims=True))
        d_logit_bf = d_logit.astype(jnp.bfloat16)
        dwr_new = dwr_acc + jnp.dot(x_dev.T, d_logit_bf, preferred_element_type=jnp.float32)
        dx_dev = (dx_expert + jnp.dot(d_logit_bf, w_router.T, preferred_element_type=jnp.float32)).astype(jnp.bfloat16)
        return (dwg_new, dwu_new, dwd_new, dwr_new), (y_dev, dx_dev)

    init_acc = (
        jnp.zeros((NUM_EXPERTS, MODEL_DIM, FF_DIM), jnp.float32),
        jnp.zeros((NUM_EXPERTS, MODEL_DIM, FF_DIM), jnp.float32),
        jnp.zeros((NUM_EXPERTS, FF_DIM, MODEL_DIM), jnp.float32),
        jnp.zeros((MODEL_DIM, NUM_EXPERTS), jnp.float32),
    )
    dev_inputs = (
        x_tokens.reshape(NUM_DEVICES, TOK_PER_DEV, MODEL_DIM),
        router_prob.reshape(NUM_DEVICES, TOK_PER_DEV, NUM_EXPERTS),
        topk_idx.reshape(NUM_DEVICES, TOK_PER_DEV, TOP_K),
        dy_tokens.reshape(NUM_DEVICES, TOK_PER_DEV, MODEL_DIM),
    )
    final_acc, dev_outs = lax.scan(device_step, init_acc, dev_inputs)
    y_tokens = dev_outs[0].reshape(ALL_TOKENS, MODEL_DIM)
    dx_tokens = dev_outs[1].reshape(ALL_TOKENS, MODEL_DIM)
    return (y_tokens, aux_loss, dx_tokens, final_acc[3], final_acc[0], final_acc[1], final_acc[2])
```

```python
import functools

import jax
import jax.numpy as jnp
from jax import lax
from jax.experimental import pallas as pl
from jax.experimental.pallas import tpu as pltpu
from jax.sharding import PartitionSpec as P

AUX_COEF = 0.001
SLOT = 64
TILE = 512
VMEM_LIMIT = 56 * 1024 * 1024
NT = (((1,), (1,)), ((), ()))
TN = (((0,), (0,)), ((), ()))
NN = (((1,), (0,)), ((), ()))
CORE, LINK_X, LINK_Y = 1, 2, 4
F32, BF16 = jnp.float32, jnp.bfloat16


def dot(a, b, dims=NN):
    return lax.dot_general(a, b, dims, preferred_element_type=F32)


def params(*sem):
    return pltpu.CompilerParams(dimension_semantics=sem, vmem_limit_bytes=VMEM_LIMIT)


def cost(flops, byts):
    return pl.CostEstimate(flops=int(flops), bytes_accessed=int(byts), transcendentals=0)


def full(shape):
    zeros = (0,) * len(shape)
    return pl.BlockSpec(shape, lambda *_: zeros)


def hot(row, tok):
    return lax.broadcasted_iota(jnp.int32, (SLOT, tok), 0) == row


def fwd_kernel(n, capacity, *refs):
    xs = refs[: 2 * n]
    idx_ref, wrt_ref, wg_ref, wu_ref, wd_ref = refs[2 * n : 2 * n + 5]
    p_ref, pos_ref, psel_ref, wsel_ref, xg_ref, g_ref, u_ref, h_ref, os_ref, op_ref = refs[2 * n + 5 :]
    me = lax.axis_index("ep")
    e = pl.program_id(0)
    n_exp, tok = p_ref.shape[1:]
    half = tok // 2

    @pl.when(e == 0)
    def _():
        tri = (lax.broadcasted_iota(jnp.int32, (tok, tok), 0) < lax.broadcasted_iota(jnp.int32, (tok, tok), 1)).astype(F32).astype(BF16)
        ids = lax.broadcasted_iota(jnp.int32, (n_exp, tok), 0)
        mine = pl.multiple_of(me * 8, 8)
        other = pl.multiple_of((me ^ CORE) * 8, 8)
        for i in range(n):
            logits = jnp.concatenate([dot(wrt_ref[...], xs[2 * i + b][...], NT) for b in range(2)], axis=1)
            ex = jnp.exp(logits - jnp.max(logits, axis=0, keepdims=True))
            prob = ex / jnp.sum(ex, axis=0, keepdims=True)
            mask = ids == idx_ref[i, 0:1, :]
            for k in range(1, 6):
                mask = jnp.logical_or(mask, ids == idx_ref[i, k : k + 1, :])
            pick = jnp.where(mask, prob, 0.0)
            gate = pick / jnp.sum(pick, axis=0, keepdims=True)
            earlier = dot(mask.astype(F32).astype(BF16), tri).astype(jnp.int32)
            pos = jnp.where(mask, jnp.where(earlier < capacity, earlier, tok), -1)
            p_ref[i] = prob
            pos_ref[i] = pos
            psel_ref[i, 0:8, :] = pos_ref[i, pl.ds(mine, 8), :]
            psel_ref[i, 8:16, :] = pos_ref[i, pl.ds(other, 8), :]
            wsel_ref[i, 0:n_exp, :] = gate.astype(BF16).astype(F32)
            top = wsel_ref[i, pl.ds(mine, 8), :]
            bot = wsel_ref[i, pl.ds(other, 8), :]
            wsel_ref[i, 0:8, :] = top
            wsel_ref[i, 8:16, :] = bot

    rows = []
    for i in range(n):
        sel = hot(psel_ref[i, pl.ds(e, 1), :], tok).astype(F32).astype(BF16)
        rows.append((dot(sel[:, :half], xs[2 * i][...]) + dot(sel[:, half:], xs[2 * i + 1][...])).astype(BF16))
    xe = jnp.concatenate(rows, axis=0)
    xg_ref[0] = xe
    g = dot(xe, wg_ref[0])
    u = dot(xe, wu_ref[0])
    h = (g * jax.nn.sigmoid(g) * u).astype(BF16)
    g_ref[0] = g
    u_ref[0] = u
    h_ref[0] = h
    o = dot(h, wd_ref[0]).astype(BF16)
    for i in range(n):
        (os_ref if i % 2 == 0 else op_ref)[i // 2, 0] = o[i * SLOT : (i + 1) * SLOT]


def piece_specs(pieces, width):
    return [pl.BlockSpec((pieces[0][2], width), lambda e, b=b: (b, 0)) for _, b, _ in pieces]


def fwd_chunk(pieces, idx, first, wrt, wg, wu, wd, capacity):
    n = len(pieces) // 2
    n_loc, dim, ff = wg.shape
    n_exp = wrt.shape[0]
    tok = idx.shape[2]
    m = n * SLOT
    in_specs = piece_specs(pieces, dim) + [
        pl.BlockSpec((n, 8, tok), lambda e: (first // n, 0, 0)),
        full((n_exp, dim)),
        pl.BlockSpec((1, dim, ff), lambda e: (e, 0, 0)),
        pl.BlockSpec((1, dim, ff), lambda e: (e, 0, 0)),
        pl.BlockSpec((1, ff, dim), lambda e: (e, 0, 0)),
    ]
    half_out = pl.BlockSpec((n // 2, 1, SLOT, dim), lambda e: (0, e, 0, 0))
    row_out = lambda w: pl.BlockSpec((1, m, w), lambda e: (e, 0, 0))
    out_shape = [
        jax.ShapeDtypeStruct((n, n_exp, tok), F32),
        jax.ShapeDtypeStruct((n, n_exp, tok), jnp.int32),
        jax.ShapeDtypeStruct((n, 16, tok), jnp.int32),
        jax.ShapeDtypeStruct((n, n_exp, tok), F32),
        jax.ShapeDtypeStruct((n_loc, m, dim), BF16),
        jax.ShapeDtypeStruct((n_loc, m, ff), F32),
        jax.ShapeDtypeStruct((n_loc, m, ff), F32),
        jax.ShapeDtypeStruct((n_loc, m, ff), BF16),
        jax.ShapeDtypeStruct((n // 2, n_loc, SLOT, dim), BF16),
        jax.ShapeDtypeStruct((n // 2, n_loc, SLOT, dim), BF16),
    ]
    out_specs = [full(s.shape) for s in out_shape[:4]] + [row_out(dim), row_out(ff), row_out(ff), row_out(ff), half_out, half_out]
    return pl.pallas_call(
        functools.partial(fwd_kernel, n, capacity),
        grid=(n_loc,),
        in_specs=in_specs,
        out_specs=out_specs,
        out_shape=out_shape,
        compiler_params=params("arbitrary"),
        cost_estimate=cost(n_loc * (6 * m * dim * ff + 2 * m * tok * dim), 3 * 2 * n_loc * dim * ff + n_loc * m * dim * 8),
        name="expert_fwd",
    )(*[a for a, _, _ in pieces], idx, wrt, wg, wu, wd)


def bwd_kernel(srcs, *refs):
    n = len(srcs)
    dys = refs[: 2 * n]
    psel_ref, wsel_ref, g_ref, u_ref, os_ref, op_ref, wg_ref, wu_ref, wd_ref = refs[2 * n : 2 * n + 9]
    d_ref, dg_ref, du_ref, dxs_ref, dxp_ref, a_ref = refs[2 * n + 9 :]
    e = pl.program_id(0)
    tok = psel_ref.shape[2]
    half = tok // 2
    lane = lax.broadcasted_iota(jnp.int32, a_ref.shape, 1)

    @pl.when(e == 0)
    def _():
        a_ref[...] = jnp.zeros_like(a_ref)

    rows = []
    for i, r in enumerate(srcs):
        eq = hot(psel_ref[i, pl.ds(e, 1), :], tok)
        sel = eq.astype(F32).astype(BF16)
        dyg = dot(sel[:, :half], dys[2 * i][...]) + dot(sel[:, half:], dys[2 * i + 1][...])
        w_slot = jnp.sum(jnp.where(eq, wsel_ref[i, pl.ds(e, 1), :], 0.0), axis=1, keepdims=True)
        o = (os_ref if i % 2 == 0 else op_ref)[i // 2, 0].astype(F32)
        a = jnp.sum(o * dyg, axis=1, keepdims=True)
        a_ref[...] = jnp.where(lane == r * 8 + e, a, a_ref[...])
        rows.append((w_slot * dyg).astype(BF16))
    d = jnp.concatenate(rows, axis=0)
    d_ref[0] = d
    dh = dot(d, wd_ref[0], NT).astype(BF16).astype(F32)
    g = g_ref[0]
    s = jax.nn.sigmoid(g)
    dg = (dh * u_ref[0] * s * (1.0 + g * (1.0 - s))).astype(BF16)
    du = (dh * (g * s)).astype(BF16)
    dg_ref[0] = dg
    du_ref[0] = du
    dx = (dot(dg, wg_ref[0], NT) + dot(du, wu_ref[0], NT)).astype(BF16)
    for i in range(n):
        (dxs_ref if i % 2 == 0 else dxp_ref)[i // 2, 0] = dx[i * SLOT : (i + 1) * SLOT]


def bwd_chunk(srcs, pieces, psel, wsel, g, u, o_s, o_p, wg, wu, wd):
    n = len(srcs)
    n_loc, dim, ff = wg.shape
    tok = psel.shape[2]
    m = n * SLOT
    half_spec = pl.BlockSpec((n // 2, 1, SLOT, dim), lambda e: (0, e, 0, 0))
    row = lambda w: pl.BlockSpec((1, m, w), lambda e: (e, 0, 0))
    in_specs = piece_specs(pieces, dim) + [
        full((n, 16, tok)),
        pl.BlockSpec((n, 16, tok), lambda e: (0, 0, 0)),
        row(ff),
        row(ff),
        half_spec,
        half_spec,
        pl.BlockSpec((1, dim, ff), lambda e: (e, 0, 0)),
        pl.BlockSpec((1, dim, ff), lambda e: (e, 0, 0)),
        pl.BlockSpec((1, ff, dim), lambda e: (e, 0, 0)),
    ]
    out_shape = [
        jax.ShapeDtypeStruct((n_loc, m, dim), BF16),
        jax.ShapeDtypeStruct((n_loc, m, ff), BF16),
        jax.ShapeDtypeStruct((n_loc, m, ff), BF16),
        jax.ShapeDtypeStruct((n // 2, n_loc, SLOT, dim), BF16),
        jax.ShapeDtypeStruct((n // 2, n_loc, SLOT, dim), BF16),
        jax.ShapeDtypeStruct((SLOT, 128), F32),
    ]
    return pl.pallas_call(
        functools.partial(bwd_kernel, srcs),
        grid=(n_loc,),
        in_specs=in_specs,
        out_specs=[row(dim), row(ff), row(ff), half_spec, half_spec, full((SLOT, 128))],
        out_shape=out_shape,
        compiler_params=params("arbitrary"),
        cost_estimate=cost(n_loc * (6 * m * dim * ff + 2 * m * tok * dim), 3 * 2 * n_loc * dim * ff + n_loc * m * dim * 10),
        name="expert_bwd",
    )(*[a for a, _, _ in pieces], psel, wsel, g, u, o_s, o_p, wg, wu, wd)


def comb_kernel(halves, weighted, n_adds, has_dz, *refs):
    psel_ref, wsel_ref, om_ref, op_ref = refs[:4]
    adds = refs[4 : 4 + n_adds]
    dz_ref, wrt_ref = refs[4 + n_adds : 6 + n_adds] if has_dz else (None, None)
    out_ref, ct_ref = refs[-2:]
    hs = psel_ref.shape[2] // 2
    per = n_adds // len(halves)
    n_loc = om_ref.shape[1]

    @pl.when(pl.program_id(0) == 0)
    def _():
        for j, hf in enumerate(halves):
            cols = slice(hf * hs, (hf + 1) * hs)
            for e in range(2 * n_loc):
                val = wsel_ref[0, e : e + 1, cols] if weighted else 1.0
                c = jnp.where(hot(psel_ref[0, e : e + 1, cols], hs), val, 0.0).astype(BF16)
                ct_ref[e * SLOT : (e + 1) * SLOT, j * hs : (j + 1) * hs] = c

    om = om_ref[0].reshape(n_loc * SLOT, om_ref.shape[3])
    op = op_ref[0].reshape(n_loc * SLOT, om_ref.shape[3])
    for j, hf in enumerate(halves):
        cols = slice(j * hs, (j + 1) * hs)
        acc = dot(ct_ref[: n_loc * SLOT, cols], om, TN) + dot(ct_ref[n_loc * SLOT :, cols], op, TN)
        for k in range(per):
            acc = acc + adds[j * per + k][...]
        if has_dz:
            acc = acc + dot(dz_ref[0, :, hf * hs : (hf + 1) * hs], wrt_ref[...], TN)
        out_ref[cols, :] = acc.astype(out_ref.dtype)


def comb(halves, psel, wsel, i, om, op, io, adds=(), dz=None, wrt=None, weighted=True, out=F32):
    _, n_loc, _, dim = om.shape
    tok = psel.shape[2]
    hs = tok // 2
    rows = hs * len(halves)
    sel_spec = lambda: pl.BlockSpec((1, 16, tok), lambda c: (i, 0, 0))
    o_spec = lambda: pl.BlockSpec((1, n_loc, SLOT, TILE), lambda c: (io, 0, 0, c))
    in_specs = [sel_spec(), sel_spec(), o_spec(), o_spec()] + [pl.BlockSpec((hs, TILE), lambda c: (0, c)) for _ in adds]
    args = [psel, wsel, om, op, *adds]
    if dz is not None:
        in_specs += [pl.BlockSpec((1, dz.shape[1], tok), lambda c: (0, 0, 0)), pl.BlockSpec((wrt.shape[0], TILE), lambda c: (0, c))]
        args += [dz, wrt]
    return pl.pallas_call(
        functools.partial(comb_kernel, halves, weighted, len(adds), dz is not None),
        grid=(dim // TILE,),
        in_specs=in_specs,
        out_specs=pl.BlockSpec((rows, TILE), lambda c: (0, c)),
        out_shape=jax.ShapeDtypeStruct((rows, dim), out),
        scratch_shapes=[pltpu.VMEM((2 * n_loc * SLOT, rows), BF16)],
        compiler_params=params("arbitrary"),
        cost_estimate=cost(4 * rows * n_loc * SLOT * dim, 4 * n_loc * SLOT * dim + 4 * rows * dim * (1 + len(adds))),
        name="combine",
    )(*args)


def wgrad_kernel(n_chunk, *refs):
    xg, dg, du, h, d = (refs[i * n_chunk : (i + 1) * n_chunk] for i in range(5))
    wg_ref, wu_ref, wd_ref = refs[5 * n_chunk :]
    cat = lambda rs: jnp.concatenate([r[0] for r in rs], axis=0)
    x = cat(xg)
    wg_ref[0] = dot(x, cat(dg), TN)
    wu_ref[0] = dot(x, cat(du), TN)
    wd_ref[0] = dot(cat(h), cat(d), TN)


def wgrad(xg, dg, du, h, d):
    groups = (xg, dg, du, h, d)
    n_loc, _, dim = xg[0].shape
    ff = h[0].shape[2]
    spec = lambda a: pl.BlockSpec((1,) + a.shape[1:], lambda e: (e, 0, 0))
    rows = sum(a.shape[1] for a in xg)
    return pl.pallas_call(
        functools.partial(wgrad_kernel, len(xg)),
        grid=(n_loc,),
        in_specs=[spec(a) for grp in groups for a in grp],
        out_specs=[
            pl.BlockSpec((1, dim, ff), lambda e: (e, 0, 0)),
            pl.BlockSpec((1, dim, ff), lambda e: (e, 0, 0)),
            pl.BlockSpec((1, ff, dim), lambda e: (e, 0, 0)),
        ],
        out_shape=[
            jax.ShapeDtypeStruct((n_loc, dim, ff), F32),
            jax.ShapeDtypeStruct((n_loc, dim, ff), F32),
            jax.ShapeDtypeStruct((n_loc, ff, dim), F32),
        ],
        compiler_params=params("arbitrary"),
        cost_estimate=cost(n_loc * 6 * rows * dim * ff, n_loc * (12 * dim * ff + 4 * rows * dim + 6 * rows * ff)),
        name="expert_wgrad",
    )(*[a for grp in groups for a in grp])


def route_kernel(n_total, p_ref, pos_ref, a_ref, dz_ref, aux_ref, frac_ref, at_ref):
    me = lax.axis_index("ep")
    r = pl.program_id(0)
    n_dev, n_exp, tok = p_ref.shape

    @pl.when(r == 0)
    def _():
        cnt = jnp.zeros((n_exp, 1), F32)
        mean = jnp.zeros((n_exp, 1), F32)
        for s in range(n_dev):
            src = me ^ s
            cnt = cnt + jnp.sum(jnp.where(pos_ref[src] >= 0, 1.0, 0.0), axis=1, keepdims=True)
            mean = mean + jnp.sum(p_ref[src], axis=1, keepdims=True)
        frac = cnt / (n_total * 6)
        frac_ref[...] = jnp.broadcast_to(frac, frac_ref.shape)
        aux_ref[...] = jnp.broadcast_to(AUX_COEF * n_exp * jnp.sum(frac * (mean / n_total), axis=0, keepdims=True), aux_ref.shape)

    for ro in range(n_dev):
        base = pl.multiple_of((me ^ ro) * 8, 8)
        here = pos_ref[r, pl.ds(base, 8), :]
        cols = pltpu.roll(a_ref[ro], 128 - 8 * (r ^ ro), 1)
        out = []
        for e in range(8):
            out.append(jnp.sum(jnp.where(hot(here[e : e + 1, :], tok), cols[:, e : e + 1], 0.0), axis=0, keepdims=True))
        at_ref[pl.ds(base, 8), :] = jnp.concatenate(out, axis=0)

    prob = p_ref[r]
    mask = pos_ref[r] >= 0
    pick = jnp.where(mask, prob, 0.0)
    total = jnp.sum(pick, axis=0, keepdims=True)
    a = at_ref[...]
    inner = jnp.sum(a * (pick / total), axis=0, keepdims=True)
    q = jnp.where(mask, (a - inner) / total, 0.0) + AUX_COEF * n_exp * frac_ref[:, 0:1] / n_total
    dz_ref[0] = (prob * (q - jnp.sum(prob * q, axis=0, keepdims=True))).astype(BF16)


def route_bwd(prob, pos, a_all, n_total):
    n_dev, n_exp, tok = prob.shape
    return pl.pallas_call(
        functools.partial(route_kernel, n_total),
        grid=(n_dev,),
        in_specs=[full(prob.shape), full(pos.shape), full(a_all.shape)],
        out_specs=[pl.BlockSpec((1, n_exp, tok), lambda r: (r, 0, 0)), full((8, 128))],
        out_shape=[jax.ShapeDtypeStruct((n_dev, n_exp, tok), BF16), jax.ShapeDtypeStruct((8, 128), F32)],
        scratch_shapes=[pltpu.VMEM((n_exp, 128), F32), pltpu.VMEM((n_exp, tok), F32)],
        compiler_params=params("arbitrary"),
        cost_estimate=cost(1e10, 4e6),
        name="route_bwd",
    )(prob, pos, a_all)


def dwr_kernel(n_dev, *refs):
    dz_ref = refs[0]
    xs = refs[1 : 1 + 2 * n_dev]
    out_ref, buf_ref = refs[-2:]
    me = lax.axis_index("ep")
    half = dz_ref.shape[2] // 2
    for r in range(n_dev):
        buf_ref[r] = dot(dz_ref[r, :, :half], xs[2 * r][...]) + dot(dz_ref[r, :, half:], xs[2 * r + 1][...])
    acc = buf_ref[me]
    for s in range(1, n_dev):
        acc = acc + buf_ref[me ^ s]
    out_ref[...] = acc


def dwr_sum(dz, pieces):
    n_dev, n_exp, tok = dz.shape
    dim = pieces[0][0].shape[1]
    tile = TILE
    return pl.pallas_call(
        functools.partial(dwr_kernel, n_dev),
        grid=(dim // tile,),
        in_specs=[full(dz.shape)] + [pl.BlockSpec((hs, tile), lambda c, b=b: (b, c)) for _, b, hs in pieces],
        out_specs=pl.BlockSpec((n_exp, tile), lambda c: (0, c)),
        out_shape=jax.ShapeDtypeStruct((n_exp, dim), F32),
        scratch_shapes=[pltpu.VMEM((n_dev, n_exp, tile), F32)],
        compiler_params=params("arbitrary"),
        cost_estimate=cost(2 * n_dev * n_exp * tok * dim, 2 * n_dev * tok * dim),
        name="router_wgrad",
    )(dz, *[a for a, _, _ in pieces])


def solution(mesh):
    n_dev = mesh.shape["ep"]

    def send(v, hop):
        return lax.ppermute(v, "ep", [(i, i ^ hop) for i in range(n_dev)])

    def spread(v):
        v = jnp.concatenate([v, send(v, CORE)], axis=0)
        v1 = v
        v = jnp.concatenate([v, send(v, LINK_X)], axis=0)
        return v1, jnp.concatenate([v, send(v, LINK_Y)], axis=0)

    def gather_rows(v, after=()):
        hs = v.shape[0] // 2
        got = {(0, 0): (v, 0, hs), (0, 1): (v, 1, hs)}
        core = send(v, CORE)
        got[1, 0], got[1, 1] = (core, 0, hs), (core, 1, hs)
        if after:
            v = lax.optimization_barrier((v, *after))[0]
        lo, hi = v[:hs], v[hs:]
        x_lo, y_hi = send(lo, LINK_X), send(hi, LINK_Y)
        x_hi, y_lo = send(hi, LINK_X), send(lo, LINK_Y)
        d_lo, d_hi = send(x_lo, LINK_Y), send(y_hi, LINK_X)
        for r, parts in ((2, (x_lo, x_hi)), (4, (y_lo, y_hi)), (6, (d_lo, d_hi))):
            for b, part in enumerate(parts):
                got[r, b] = (part, 0, hs)
                got[r + 1, b] = (send(part, CORE), 0, hs)
        return [[got[r, b] for b in range(2)] for r in range(8)], (x_hi, y_lo)

    def local_block(x_loc, w_router, wg, wu, wd, idx_loc, dy_loc):
        tok, dim = x_loc.shape
        top_k = idx_loc.shape[1]
        n_exp = w_router.shape[1]
        capacity = (5 * tok * top_k + 4 * n_exp - 1) // (4 * n_exp)
        wrt = w_router.T
        idx_t = jnp.pad(idx_loc.T, ((0, 8 - top_k), (0, 0)), constant_values=-1)[None]
        idx1, idx_all = spread(idx_t)
        xs, x_done = gather_rows(x_loc)
        dys, _ = gather_rows(dy_loc, x_done)
        chunks = ((0, 1), (2, 3, 4, 5), (6, 7))
        where = {r: (c, i) for c, rs in enumerate(chunks) for i, r in enumerate(rs)}

        fwd = []
        for c, rs in enumerate(chunks):
            pieces = [p for r in rs for p in xs[r]]
            idx = idx1 if c == 0 else idx_all[rs[0] : rs[-1] + 1]
            fwd.append(fwd_chunk(pieces, idx, 0, wrt, wg, wu, wd, capacity))
        prob = jnp.concatenate([f[0] for f in fwd], axis=0)
        pos = jnp.concatenate([f[1] for f in fwd], axis=0)

        def reduce_back(mine, theirs, weighted, dz=None, out=BF16):
            def part(r, halves, **kw):
                c, i = where[r]
                return comb(halves, fwd[c][2], fwd[c][3], i, mine[c], theirs[c], i // 2, weighted=weighted, **kw)

            x_d = send(part(6, (0,)), LINK_X)
            y_d = send(part(6, (1,)), LINK_Y)
            x_a = send(part(2, (0,)), LINK_X)
            y_b = send(part(4, (1,)), LINK_Y)
            y_a = send(part(4, (0,), adds=(x_d,)), LINK_Y)
            x_b = send(part(2, (1,), adds=(y_d,)), LINK_X)
            extra = {} if dz is None else {"dz": dz, "wrt": wrt}
            return part(0, (0, 1), adds=(x_a, y_a, x_b, y_b), out=out, **extra)

        o_mine = [f[8] for f in fwd]
        o_theirs = [send(f[9], CORE) for f in fwd]
        y_loc = reduce_back(o_mine, o_theirs, True)

        bwd = []
        for c, rs in enumerate(chunks):
            pieces = [p for r in rs for p in dys[r]]
            f = fwd[c]
            bwd.append(bwd_chunk(rs, pieces, f[2], f[3], f[5], f[6], f[8], f[9], wg, wu, wd))
        a_part = bwd[0][5] + bwd[1][5] + bwd[2][5]
        _, a_all = spread(a_part[None])
        dz, aux = route_bwd(prob, pos, a_all, tok * n_dev)
        dx_mine = [b[3] for b in bwd]
        dx_theirs = [send(b[4], CORE) for b in bwd]
        dx_loc = reduce_back(dx_mine, dx_theirs, False, dz=dz)
        dw_router = dwr_sum(dz, [p for r in range(8) for p in xs[r]]).T
        dwg, dwu, dwd = wgrad([f[4] for f in fwd], [b[1] for b in bwd], [b[2] for b in bwd], [f[7] for f in fwd], [b[0] for b in bwd])
        return y_loc, aux[0, 0], dx_loc, dw_router, dwg, dwu, dwd

    tok_spec = P("ep")
    return jax.shard_map(
        local_block,
        mesh=mesh,
        in_specs=(tok_spec, P(), tok_spec, tok_spec, tok_spec, tok_spec, tok_spec),
        out_specs=(tok_spec, P(), tok_spec, P(), tok_spec, tok_spec, tok_spec),
        check_vma=False,
    )
```
